32 devices in a mesh: bank: 8 (over z, core), zero: 4 (over y, x).
Axes of the slice: x: 2, y: 2, z: 4, core: 2. Of those that a mesh axis runs over, the one named last changes fastest.
Arguments:
- master_down: float32 [64, 1024, 2048], P('bank', None, 'zero'), may hold values from -0.25 to 0.25
- second_down: bfloat16 [64, 1024, 2048], P('bank', None, 'zero'), may hold values from -0.09375 to 0.09375
- router_weight: float32 [2048, 64], P('zero', 'bank'), may hold values from -0.125 to 0.125
- router_gain: float32 [2048], P('zero'), may hold values from 0.25 to 1.75
Outputs:
- final_down: bfloat16 [64, 1024, 2048], P('bank')
- scale_down: float32 [64, 1024], P('bank')
- serve_router: bfloat16 [2048, 64], replicated
The draws below stay inside these ranges and needn't reach their ends.
All inputs are finite; a program needn't handle non-finite values. Where the reference program divides by a largest or mean magnitude, that divisor is 1e-20 or more.
Results may differ from the reference program's by a relative error of at most 0.001.
Values may be sent and summed in bfloat16 or wider, within the bound.
A program may use at most 128 MiB of HBM per device.

```python
import jax
import jax.numpy as jnp

EXPERTS = 64
D_MODEL = 2048
D_EXPERT = 1024


def with_spikes(values, own_key, source, target, shards_of, factor):
    def block_of(position):
        return (jnp.arange(values.shape[position]) // (values.shape[position] // shards_of)).reshape((-1,) + (1,) * (values.ndim - 1 - position))

    near = jax.random.permutation(own_key, shards_of)[block_of(target)]
    second = (block_of(target) + shards_of // 2) % shards_of
    return jnp.where((block_of(source) == near) | (block_of(source) == second), factor * values, values)


def steps_of(stream_key, extent, cuts, least, top_value):
    factor_of, own = 1.0, jax.random.fold_in(stream_key, 6)
    for axis_at, parts in cuts:
        draws = jnp.exp(jax.random.uniform(jax.random.fold_in(own, axis_at), (parts,), jnp.float32, least / len(cuts), top_value / len(cuts)))
        factor_of = factor_of * jnp.repeat(draws, extent[axis_at] // parts).reshape([-1 if axis == axis_at else 1 for axis in range(len(extent))])
    return factor_of


def bell_draw(stream_key, shape, deviation, reach, split=(), dtype=jnp.bfloat16):
    factor_of = steps_of(stream_key, shape, split, -0.22, 0.18) if split else 1.0
    entries = jax.random.normal(stream_key, shape, jnp.float32) * deviation * factor_of
    return jnp.minimum(jnp.maximum(entries, -reach), reach).astype(dtype)


def noise_with(key, dims, width, bound, split, heavy, kind=jnp.bfloat16):
    entries = width * jax.random.normal(key, dims, jnp.float32)
    if split:
        entries = entries * steps_of(key, dims, split, -0.22, 0.18)
    return jnp.clip(with_spikes(entries, jax.random.fold_in(key, 3), *heavy), -bound, bound).astype(kind)


def setup_inputs(seed: int = 0) -> dict:
    key_of = jax.random.split(jax.random.key(seed), 5)
    master_down = noise_with(key_of[0], (EXPERTS, D_EXPERT, D_MODEL), D_EXPERT ** -0.5, 0.25, ((0, 8), (2, 4)), (2, 1, 4, 2.0), jnp.float32)
    second_down = bell_draw(key_of[1], (EXPERTS, D_EXPERT, D_MODEL), (D_EXPERT * 4) ** -0.5, 0.09375, ((0, 8), (2, 4)))
    router_weight = bell_draw(key_of[2], (D_MODEL, EXPERTS), D_MODEL ** -0.5, 0.125, ((0, 4), (1, 8)), jnp.float32)
    router_gain = jnp.clip(1.0 + 0.15 * jax.random.normal(key_of[3], (D_MODEL,), jnp.float32), 0.25, 1.75)
    return {"master_down": master_down, "second_down": second_down, "router_weight": router_weight, "router_gain": router_gain}


def reference(master_down, second_down, router_weight, router_gain):
    merged_down = master_down + second_down.astype(jnp.float32)
    scale_down = jnp.max(jnp.abs(merged_down), axis=2)
    final_down = (merged_down / jnp.expand_dims(scale_down, 2)).astype(jnp.bfloat16)
    serve_router = (router_weight * router_gain[:, None]).astype(jnp.bfloat16)
    return final_down, scale_down, serve_router
```

```python
import functools
import math

import jax
import jax.numpy as jnp
from jax import lax
from jax.experimental import pallas as pl
from jax.experimental.pallas import tpu as pltpu
from jax.sharding import PartitionSpec as P


LANES = 128


def ring_order(size):
    side = math.isqrt(size)
    if side * side != size or side % 2:
        return list(range(size))
    cycle = [row * side for row in range(side)]
    for row in reversed(range(side)):
        columns = range(1, side)
        if (side - 1 - row) % 2:
            columns = reversed(columns)
        cycle += [row * side + column for column in columns]
    return cycle


def place_kernel(count, experts, steps, fresh, column_ref, *refs):
    pieces = refs[:count]
    out = refs[count + (0 if fresh else 1)]
    held, in_sem, out_sem = refs[-3:]
    width = held.shape[-1]

    def copy_in(at):
        return pltpu.make_async_copy(pieces[at], held.at[pl.ds(at, 1)], in_sem.at[at])

    def copy_out(at):
        column = pl.multiple_of(column_ref[steps[at]] * width, width)
        return pltpu.make_async_copy(held.at[pl.ds(at, 1)], out.at[pl.ds(experts[at], 1), :, pl.ds(column, width)], out_sem.at[at])

    for at in range(count):
        copy_in(at).start()
    for at in range(count):
        copy_in(at).wait()
        copy_out(at).start()
    for at in range(count):
        copy_out(at).wait()


def place(out, shape, pieces, experts, steps, columns):
    count = len(pieces)
    fresh = out is None
    piece = pieces[0]
    operands = list(pieces) + ([] if fresh else [out])
    return pl.pallas_call(
        functools.partial(place_kernel, count, tuple(experts), tuple(steps), fresh),
        out_shape=jax.ShapeDtypeStruct(shape, piece.dtype),
        in_specs=[pl.BlockSpec(memory_space=pltpu.SMEM)] + [pl.BlockSpec(memory_space=pl.ANY)] * len(operands),
        out_specs=pl.BlockSpec(memory_space=pl.ANY),
        scratch_shapes=[
            pltpu.VMEM((count,) + piece.shape[1:], piece.dtype),
            pltpu.SemaphoreType.DMA((count,)),
            pltpu.SemaphoreType.DMA((count,)),
        ],
        input_output_aliases={} if fresh else {1 + count: 0},
        cost_estimate=pl.CostEstimate(flops=0, transcendentals=0, bytes_accessed=2 * count * piece.size * 2),
    )(columns, *operands)


def blocks_of(array, start):
    return [array[pl.ds(start, LANES), column : column + LANES] for column in range(0, array.shape[-1], LANES)]


def first_kernel(size, master, second, router, gain, scale, rows_router, narrow, wide, change, mine, others, part, parts, wide_sem, change_sem, send_sem, recv_sem, route_send, route_recv):
    local, rows, _ = master.shape
    me = lax.axis_index("zero")
    peers = [lax.rem(me + step, size) for step in range(1, size)]
    barrier = pltpu.get_barrier_semaphore()
    for peer in peers:
        pl.semaphore_signal(barrier, inc=1, device_id={"zero": peer}, device_id_type=pl.DeviceIdType.MESH)

    def load(e):
        return (
            pltpu.make_async_copy(master.at[e], wide.at[e], wide_sem.at[e]),
            pltpu.make_async_copy(second.at[e], change.at[e], change_sem.at[e]),
        )

    def send(source, target, step, out_sem, in_sem):
        return pltpu.make_async_remote_copy(
            src_ref=source,
            dst_ref=target.at[me],
            send_sem=out_sem.at[step],
            recv_sem=in_sem.at[step],
            device_id={"zero": peers[step]},
            device_id_type=pl.DeviceIdType.MESH,
        )

    for e in range(local):
        for copy in load(e):
            copy.start()
    part[...] = (router[...] * gain[...]).astype(part.dtype)

    for e in range(local):
        for copy in load(e):
            copy.wait()
        for start in range(0, rows, LANES):
            top = None
            for base, delta in zip(blocks_of(wide.at[e], start), blocks_of(change.at[e], start)):
                block = jnp.abs(base + delta.astype(jnp.float32))
                top = block if top is None else jnp.maximum(top, block)
            mine[e : e + 1, start : start + LANES] = jnp.max(top.T, axis=0, keepdims=True)
    pl.semaphore_wait(barrier, size - 1)
    sent = []
    for step in range(size - 1):
        sent.append(send(mine, others, step, send_sem, recv_sem))
    for step in range(size - 1):
        sent.append(send(part, parts, step, route_send, route_recv))
    for copy in sent:
        copy.start()
    rows_router[me] = part[...]
    for copy in sent[: size - 1]:
        copy.wait_recv()
    top = mine[...]
    for step in range(1, size):
        top = jnp.maximum(top, others[lax.rem(me + size - step, size)])
    scale[...] = top
    for start in range(0, rows, LANES):
        down = jnp.broadcast_to(scale[0:1, start : start + LANES], (LANES, LANES)).T
        for at, (base, delta) in enumerate(zip(blocks_of(wide.at[0], start), blocks_of(change.at[0], start))):
            ratio = (base + delta.astype(jnp.float32)) / down
            narrow[0, start : start + LANES, at * LANES : (at + 1) * LANES] = ratio.astype(narrow.dtype)
    for step, copy in enumerate(sent[size - 1 :]):
        copy.wait_recv()
        owner = lax.rem(me + size - 1 - step, size)
        rows_router[owner] = parts[owner]
    for copy in sent:
        copy.wait_send()


def first(size, master_down, second_down, router_weight, router_gain):
    local, rows, width = master_down.shape
    router = router_weight.T
    in_vmem = pl.BlockSpec(memory_space=pltpu.VMEM)
    in_hbm = pl.BlockSpec(memory_space=pl.ANY)
    return pl.pallas_call(
        functools.partial(first_kernel, size),
        out_shape=(
            jax.ShapeDtypeStruct((local, rows), jnp.float32),
            jax.ShapeDtypeStruct((size,) + router.shape, jnp.bfloat16),
            jax.ShapeDtypeStruct((1, rows, width), jnp.bfloat16),
        ),
        in_specs=[in_hbm, in_hbm, in_vmem, in_vmem],
        out_specs=(in_vmem, in_vmem, in_vmem),
        scratch_shapes=[
            pltpu.VMEM(master_down.shape, master_down.dtype),
            pltpu.VMEM(second_down.shape, second_down.dtype),
            pltpu.VMEM((local, rows), jnp.float32),
            pltpu.VMEM((size, local, rows), jnp.float32),
            pltpu.VMEM(router.shape, jnp.bfloat16),
            pltpu.VMEM((size,) + router.shape, jnp.bfloat16),
            pltpu.SemaphoreType.DMA((local,)),
            pltpu.SemaphoreType.DMA((local,)),
        ]
        + [pltpu.SemaphoreType.DMA((size - 1,))] * 4,
        compiler_params=pltpu.CompilerParams(collective_id=0, has_side_effects=True),
    )(master_down, second_down, router, router_gain[None, :])


def shards(size, master_down, second_down, router_weight, router_gain):
    local, rows, width = master_down.shape
    cycle = ring_order(size)
    ways = {
        +1: [(cycle[at], cycle[(at + 1) % size]) for at in range(size)],
        -1: [(cycle[at], cycle[(at - 1) % size]) for at in range(size)],
    }
    me = lax.axis_index("zero")
    owners = [[cycle[(cycle.index(index) + step) % size] for step in range(size)] for index in range(size)]
    columns = jnp.asarray(owners, jnp.int32)[me]

    scale_down, rows_router, narrow_first = first(size, master_down, second_down, router_weight, router_gain)
    narrow = [narrow_first] + [
        ((master_down[e : e + 1] + second_down[e : e + 1].astype(jnp.float32)) / scale_down[e : e + 1, :, None]).astype(jnp.bfloat16)
        for e in range(1, local)
    ]
    shape = (local, rows, size * width)
    out = place(None, shape, narrow, range(local), [0] * local, columns)
    held = {+1: list(narrow), -1: list(narrow)}
    for step in range(1, size // 2 + 1):
        for e in range(local):
            pieces, steps = [], []
            for way in (+1, -1):
                if 2 * step == size and (e % 2 == 0) != (way > 0):
                    continue
                held[way][e] = lax.ppermute(held[way][e], "zero", ways[way])
                pieces.append(held[way][e])
                steps.append(-way * step % size)
            out = place(out, shape, pieces, [e] * len(pieces), steps, columns)

    all_router = lax.all_gather(rows_router, "bank", axis=0)
    serve_router = all_router.transpose(1, 3, 0, 2).reshape(size * router_weight.shape[0], -1)
    return (out, scale_down, serve_router)


def solution(mesh):
    return jax.shard_map(
        functools.partial(shards, mesh.shape["zero"]),
        mesh=mesh,
        in_specs=(P("bank", None, "zero"), P("bank", None, "zero"), P("zero", "bank"), P("zero")),
        out_specs=(P("bank", None, None), P("bank", None), P()),
        check_vma=False,
    )
```
